32 devices in a mesh: gx: 4 (over z), gy: 8 (over y, x, core).
Axes of the slice: x: 2, y: 2, z: 4, core: 2. Of those that a mesh axis runs over, the one named last changes fastest.
Arguments:
- positions: float32 [3, 4, 8, 4096], P(None, 'gx', 'gy'), may hold values from 0 to 2
- velocities: float32 [3, 4, 8, 4096], P(None, 'gx', 'gy'), may hold values from -6 to 6
- mass: float32 [4, 8, 4096], P('gx', 'gy'), may hold values from 0.05 to 0.3
- stiffness: float32 [4, 8, 4096], P('gx', 'gy'), may hold values from 0.5 to 8
- counts: int32 [4, 8, 32], P('gx', 'gy'), may hold values from 32 to 128
- pairs: int32 [4096, 2], P(('gx', 'gy')), may hold values from 0 to 1023, as said below
- pair_count: int32 [32], P(('gx', 'gy')), may hold values from 32 to 128, as said below
Outputs:
- new_positions: float32 [3, 4, 8, 4096], P(None, 'gx', 'gy')
- new_velocities: float32 [3, 4, 8, 4096], P(None, 'gx', 'gy')
- density: float32 [4, 8, 4096], P('gx', 'gy')
The draws below stay inside these ranges and needn't reach their ends.
Inputs may be any that keep to these rules, and one draw needn't show every extreme that they name: `pairs`: box d's list is rows d * 128 to (d + 1) * 128 - 1, box d being (d // 8, d % 8). Its first 32 rows pair each of the box's own tiles with itself, in order. In every other row the first tile lies in a box with the same gy index and a gx index at most one away, the second tile in a box with the same gx index and a gy index at most one away. Rows may repeat. `pair_count`: some box has 128 live rows in every draw.
All inputs are finite; a program needn't handle non-finite values.
Results may differ from the reference program's by a relative error of at most 0.0001.
Values sent between devices are 32-bit elements; how exact they have to be, the bound alone decides.
No kernel may reach another device: no remote copies, remote signals or barrier semaphores. Data moves between devices by JAX's collectives and lax.ppermute only.
A program may use at most 64 MiB of HBM per device.

```python
import math
import jax
import jax.numpy as jnp
from jax import lax

TILE = 128
TILES_DEV = 32
PAIRS_MAX = 128
SLOTS = 4096
N_GX = 4
N_GY = 8


def draw_pairs(key, part):
    boxes = N_GX * N_GY
    keys = jax.random.split(jax.random.fold_in(key, 11), 4)
    box_index = jnp.arange(boxes, dtype=jnp.int32)
    box_row = box_index // N_GY
    box_column = box_index % N_GY
    extra = PAIRS_MAX - TILES_DEV
    step_row = jax.random.randint(keys[0], (boxes, extra), -1, 2)
    step_column = jax.random.randint(keys[1], (boxes, extra), -1, 2)
    first_row = jnp.clip(box_row[:, None] + step_row, 0, N_GX - 1)
    second_column = jnp.clip(box_column[:, None] + step_column, 0, N_GY - 1)
    first_slot = jax.random.randint(keys[2], (boxes, extra), 0, TILES_DEV)
    second_slot = jax.random.randint(keys[3], (boxes, extra), 0, TILES_DEV)
    first_tiles = (first_row * N_GY + box_column[:, None]) * TILES_DEV + first_slot
    second_tiles = (box_row[:, None] * N_GY + second_column) * TILES_DEV + second_slot
    own_tiles = box_index[:, None] * TILES_DEV + jnp.arange(TILES_DEV, dtype=jnp.int32)[None, :]
    first_all = jnp.concatenate([own_tiles, first_tiles], axis=1)
    second_all = jnp.concatenate([own_tiles, second_tiles], axis=1)
    return jnp.stack([first_all, second_all], axis=-1).reshape(boxes * PAIRS_MAX, 2).astype(jnp.int32)


def draw_pair_count(key, part):
    boxes = N_GX * N_GY
    keys = jax.random.split(jax.random.fold_in(key, 23), 2)
    level = jax.random.randint(keys[0], (boxes,), 0, 65)
    extra = PAIRS_MAX - TILES_DEV
    loads = TILES_DEV + extra * level * level * level // 262144
    busiest = jax.random.randint(keys[1], (), 0, boxes)
    box_index = jnp.arange(boxes, dtype=jnp.int32)
    loads = jnp.where(box_index == busiest, PAIRS_MAX, loads)
    return loads.astype(jnp.int32)


def touch_ends(result, own_key, low, largest):
    index_at = [jax.random.randint(jax.random.fold_in(own_key, axis), (), 0, length) for axis, length in enumerate(result.shape)]
    main_axis = result.shape.index(max(result.shape))
    next_to = index_at[:main_axis] + [(index_at[main_axis] + 1) % result.shape[main_axis]] + index_at[main_axis + 1:]
    return result.at[tuple(index_at)].set(low).at[tuple(next_to)].set(largest)


def block_scale(key, dims, cuts, least, top_value):
    def one(position, parts):
        heights = jax.random.uniform(jax.random.fold_in(jax.random.fold_in(key, 6), position), (parts,), jnp.float32, least / len(cuts), top_value / len(cuts))
        return jnp.repeat(jnp.exp(heights), dims[position] // parts).reshape((-1,) + (1,) * (len(dims) - position - 1))

    loudness = one(*cuts[0])
    for cut in cuts[1:]:
        loudness = loudness * one(*cut)
    return loudness


def scatter_about(stream_key, dims, spread, bound, pieces=(), kind=jnp.bfloat16):
    loudness = block_scale(stream_key, dims, pieces, -0.22, 0.18) if pieces else 1.0
    values = jax.random.normal(stream_key, dims, jnp.float32) * spread * loudness
    return jnp.minimum(jnp.maximum(values, -bound), bound).astype(kind)


def setup_inputs(seed: int = 0) -> dict:
    seeds = jax.random.split(jax.random.key(seed), 8)
    positions = jnp.clip(2.0 * jax.random.uniform(seeds[0], (3, N_GX, N_GY, SLOTS), jnp.float32) ** block_scale(seeds[0], (3, N_GX, N_GY, SLOTS), ((1, 4), (2, 8)), -0.2, 0.2), 0.0, 2.0)
    velocities = scatter_about(seeds[1], (3, N_GX, N_GY, SLOTS), 1.0, 6.0, ((1, 4), (2, 8)), jnp.float32)
    mass = jnp.clip(jnp.exp(math.log(0.3) - 1.7917595 * jax.random.uniform(seeds[2], (N_GX, N_GY, SLOTS), jnp.float32) ** block_scale(seeds[2], (N_GX, N_GY, SLOTS), ((0, 4), (1, 8)), -0.2, 0.2)), 0.05, 0.3)
    stiffness = jnp.clip(jnp.exp(math.log(8.0) - 2.7725887 * jax.random.uniform(seeds[3], (N_GX, N_GY, SLOTS), jnp.float32) ** block_scale(seeds[3], (N_GX, N_GY, SLOTS), ((0, 4), (1, 8)), -0.2, 0.2)), 0.5, 8.0)
    counts = touch_ends(jax.random.randint(seeds[4], (N_GX, N_GY, TILES_DEV), 32, 129), jax.random.fold_in(seeds[4], 1), 32, 128).astype(jnp.int32)
    pairs = draw_pairs(jax.random.fold_in(seeds[7], 71), 0)
    pair_count = draw_pair_count(jax.random.fold_in(seeds[7], 71), 0)
    return dict(positions=positions, velocities=velocities, mass=mass, stiffness=stiffness, counts=counts, pairs=pairs, pair_count=pair_count)


kernel_norm = 21.0 / (16.0 * math.pi)
viscosity = 0.1
time_step = 0.02
rest_density = 1.0

def kernel_terms(points_a, points_b):
    offset = points_a[:, :, :, None] - points_b[:, :, None, :]
    distance = jnp.sqrt(lax.optimization_barrier(jnp.sum(offset * offset, axis=0)))
    falloff = jnp.maximum(1.0 - 0.5 * distance, 0.0)
    weight = kernel_norm * falloff ** 4 * (2.0 * distance + 1.0)
    slope = -5.0 * kernel_norm * falloff ** 3
    return (offset, weight, slope)

def density_terms(points_a, points_b, mass_a, mass_b, live_rows, cross_rows):
    offset, weight, slope = kernel_terms(points_a, points_b)
    to_first = lax.optimization_barrier(jnp.sum(weight * mass_b[:, None, :], axis=2)) * live_rows[:, None]
    to_second = lax.optimization_barrier(jnp.sum(weight * mass_a[:, :, None], axis=1)) * cross_rows[:, None]
    return (to_first, to_second)

def force_terms(points_a, points_b, speed_a, speed_b, mass_a, mass_b, press_a, press_b, scale_a, scale_b, live_rows, cross_rows):
    offset, weight, slope = kernel_terms(points_a, points_b)
    push = -(press_a[:, :, None] + press_b[:, None, :])
    drag = 2.0 * viscosity / (scale_a[:, :, None] * scale_b[:, None, :])
    relative = speed_a[:, :, :, None] - speed_b[:, :, None, :]
    force = slope[None] * (push[None] * offset + drag[None] * relative)
    to_first = lax.optimization_barrier(jnp.sum(force * mass_b[None, :, None, :], axis=3)) * live_rows[None, :, None]
    to_second = -lax.optimization_barrier(jnp.sum(force * mass_a[None, :, :, None], axis=2)) * cross_rows[None, :, None]
    return (to_first, to_second)

def reference(positions, velocities, mass, stiffness, counts, pairs, pair_count):
    tile_total = N_GX * N_GY * TILES_DEV
    points = positions.reshape(3, tile_total, TILE)
    speeds = velocities.reshape(3, tile_total, TILE)
    slot_index = jnp.arange(TILE, dtype=jnp.int32)
    validity = (slot_index[None, :] < counts.reshape(tile_total, 1)).astype(jnp.float32)
    weighted = mass.reshape(tile_total, TILE) * validity
    live_flag = (jnp.arange(PAIRS_MAX, dtype=jnp.int32)[None, :] < pair_count[:, None]).astype(jnp.float32).reshape(-1)
    first_tiles = pairs[:, 0]
    second_tiles = pairs[:, 1]
    cross_flag = jnp.where(first_tiles != second_tiles, live_flag, 0.0 * live_flag)
    row_total = first_tiles.shape[0]
    block_rows = math.gcd(row_total, 256)
    block_count = row_total // block_rows
    inputs = (first_tiles.reshape(block_count, block_rows), second_tiles.reshape(block_count, block_rows), live_flag.reshape(block_count, block_rows), cross_flag.reshape(block_count, block_rows))

    def density_block(totals, block):
        first_ids, second_ids, live_rows, cross_rows = block
        to_first, to_second = density_terms(points[:, first_ids], points[:, second_ids], weighted[first_ids], weighted[second_ids], live_rows, cross_rows)
        totals = totals.at[first_ids].add(to_first).at[second_ids].add(to_second)
        return (totals, None)
    density, ignored = lax.scan(density_block, jnp.zeros((tile_total, TILE), jnp.float32), inputs)
    scale = density + 1.0 - validity
    press = stiffness.reshape(tile_total, TILE) * (density - rest_density) / (scale * scale)

    def force_block(totals, block):
        first_ids, second_ids, live_rows, cross_rows = block
        to_first, to_second = force_terms(points[:, first_ids], points[:, second_ids], speeds[:, first_ids], speeds[:, second_ids], weighted[first_ids], weighted[second_ids], press[first_ids], press[second_ids], scale[first_ids], scale[second_ids], live_rows, cross_rows)
        totals = totals.at[:, first_ids].add(to_first).at[:, second_ids].add(to_second)
        return (totals, None)
    accel, ignored = lax.scan(force_block, jnp.zeros((3, tile_total, TILE), jnp.float32), inputs)
    new_speeds = speeds + time_step * validity[None] * accel
    new_points = points + time_step * new_speeds
    return (new_points.reshape(positions.shape), new_speeds.reshape(velocities.shape), density.reshape(mass.shape))
```

```python
import functools
import math

import jax
import jax.numpy as jnp
from jax import lax
from jax.experimental import pallas as pl
from jax.experimental.pallas import tpu as pltpu
from jax.sharding import PartitionSpec as P

kernel_norm = 21.0 / (16.0 * math.pi)
viscosity = 0.1
time_step = 0.02
rest_density = 1.0
FIELDS = 8
UNROLL = 4
SHIFT = 64


def swap_routes(axis):
    count = lax.axis_size(axis)
    routes = []
    for parity in (0, 1):
        route = []
        for i in range(parity, count - 1, 2):
            route += [(i, i + 1), (i + 1, i)]
        routes.append(route)
    return routes


def swapped(block, axis):
    return [lax.ppermute(block, axis, route) for route in swap_routes(axis)]


def split_int(value, size):
    if size & (size - 1) == 0:
        return value >> (size.bit_length() - 1), value & (size - 1)
    return lax.div(value, jnp.int32(size)), lax.rem(value, jnp.int32(size))


def partner_slot(step, here):
    even = lax.rem(here, 2) == 0
    up = jnp.where(even, 1, 2)
    return jnp.where(step == 0, 0, jnp.where(step > 0, up, 3 - up))


def pack_kernel(tiles, tile_size, width_gy, where_ref, counts_ref, live_ref, points_ref, speeds_ref,
                mass_ref, pairs_ref, packed_ref, codes_ref):
    rows = pairs_ref.shape[0]
    row_here, column_here = where_ref[0], where_ref[1]
    lane = lax.broadcasted_iota(jnp.int32, (1, tile_size), 1)
    for t in range(tiles):
        for c in range(3):
            packed_ref[t, c : c + 1, :] = 0.5 * points_ref[c * tiles + t : c * tiles + t + 1, :]
            packed_ref[t, 4 + c : 5 + c, :] = speeds_ref[c * tiles + t : c * tiles + t + 1, :]
        packed_ref[t, 3:4, :] = jnp.where(lane < counts_ref[t], mass_ref[t : t + 1, :], 0.0)
        packed_ref[t, 7:8, :] = jnp.zeros((1, tile_size), jnp.float32)
    box, slot = split_int(pairs_ref[...], tiles)
    box_gx, box_gy = split_int(box, width_gy)
    side_a = partner_slot(box_gx[:, 0:1] - row_here, row_here)
    side_b = partner_slot(box_gy[:, 1:2] - column_here, column_here)
    slot_a, slot_b = slot[:, 0:1], slot[:, 1:2]
    row_index = lax.broadcasted_iota(jnp.int32, (rows, 1), 0)
    live = (row_index >= tiles) & (row_index < live_ref[0])
    cross = live & (pairs_ref[:, 0:1] != pairs_ref[:, 1:2])
    group_a = jnp.where(live, side_a, 7)
    group_b = jnp.where(cross, side_b + 3, 7)
    source_box = (side_b * 3 + side_a) * tiles
    code_a = (slot_a + SHIFT * (source_box + slot_b)).astype(jnp.float32)
    code_b = (slot_b + SHIFT * (source_box + slot_a)).astype(jnp.float32)
    lanes = lax.broadcasted_iota(jnp.int32, (rows, rows), 1)
    subs = lax.broadcasted_iota(jnp.int32, (rows, rows), 0)
    flags = jnp.where((lanes == group_a) | (lanes == group_b), 1.0, 0.0)
    flags = jnp.where(lanes < 6, flags, 0.0)
    below = jnp.where(lanes < subs, 1.0, 0.0).astype(jnp.bfloat16)
    places = jnp.dot(below, flags.astype(jnp.bfloat16), preferred_element_type=jnp.float32)
    totals = jnp.sum(flags, axis=0, keepdims=True)
    codes_ref[...] = jnp.zeros(codes_ref.shape, jnp.float32)
    for q in range(6):
        group, code = (group_a, code_a) if q < 3 else (group_b, code_b)
        place = jnp.where(group == q, places[:, q : q + 1].astype(jnp.int32), -1)
        listed = jnp.sum(jnp.where(place == lanes, code, 0.0), axis=0, keepdims=True)
        total = totals[:, q : q + 1]
        row_lane = lanes[0:1, :]
        listed = jnp.where(row_lane < total.astype(jnp.int32), listed, float(tiles))
        listed = jnp.where(row_lane == rows - 1, total, listed)
        codes_ref[q : q + 1, :] = listed
        if q not in (0, 3):
            packed_ref[q, 7:8, :] = listed


def falloffs(source, target):
    size = source.shape[0]
    for j in range(0, size, 8):
        d0 = source[j : j + 8, 0:1] - target[0:1, :]
        d1 = source[j : j + 8, 1:2] - target[1:2, :]
        d2 = source[j : j + 8, 2:3] - target[2:3, :]
        square = d0 * d0 + d1 * d1 + d2 * d2
        half = square * lax.rsqrt(jnp.maximum(square, 1e-30))
        yield j, jnp.maximum(1.0 - half, 0.0)


def density_side(source_block, target_block):
    source = source_block.T
    total = None
    for j, falloff in falloffs(source, target_block):
        f2 = falloff * falloff
        term = f2 * f2 * (1.25 - falloff) * source[j : j + 8, 3:4]
        total = term if total is None else total + term
    return total


def split_terms(values, terms):
    parts = []
    rest = values
    for i in range(terms):
        part = rest.astype(jnp.bfloat16)
        parts.append(part)
        if i + 1 < terms:
            rest = rest - part.astype(jnp.float32)
    return parts


def force_side(source_block, source_extra, target_block):
    source = source_block.T
    high, low = [], []
    held = None
    for j, falloff in falloffs(source, target_block):
        cube = falloff * falloff * falloff
        if held is None:
            held = cube
            continue
        pair = jnp.concatenate([held, cube], axis=0)
        held = None
        top, rest = split_terms(pair, 2)
        high.append(top)
        low.append(rest)
    slope = jnp.concatenate(high + low, axis=0)
    sub = lax.broadcasted_iota(jnp.int32, source_block.shape, 0)
    base = jnp.where((sub == 3) | (sub == 7), 1.0, source_block)
    mass = source_block[3:4, :]
    mass_press = mass * source_extra[0:1, :]
    mass_inverse = mass * source_extra[1:2, :]
    columns = jnp.concatenate(
        [base * jnp.where(sub < 4, mass, mass_inverse), base * mass_press], axis=0
    )
    columns = jnp.concatenate(split_terms(columns, 3), axis=0)
    columns = jnp.concatenate([columns, columns], axis=1)
    sums = jnp.dot(columns, slope, preferred_element_type=jnp.float32)
    return sums[0:16] + sums[16:32] + sums[32:48]


def each_side(codes, lists, tiles, one_side):
    limit = codes.shape[1] - 1

    def over_list(q, carry):
        trips = (codes[q, limit] + UNROLL - 1) // UNROLL

        def trip(i, inner):
            for u in range(UNROLL):
                code = codes[q, i * UNROLL + u]
                one_side(code & (SHIFT - 1), code >> (SHIFT.bit_length() - 1))
            return inner

        return lax.fori_loop(0, trips, trip, carry)

    lax.fori_loop(0, lists, over_list, 0)


def density_self_kernel(tiles, packed_ref, sums_ref):
    def trip(i, carry):
        for u in range(UNROLL):
            t = i * UNROLL + u
            block = packed_ref[t]
            sums_ref[t] = density_side(block, block)
        return carry

    lax.fori_loop(0, tiles // UNROLL, trip, 0)
    sums_ref[tiles] = jnp.zeros(sums_ref.shape[1:], jnp.float32)


def density_kernel(tiles, tile_size, counts_ref, sums_in_ref, stiff_ref, codes_in_ref, near_ref, even_ref,
                   odd_ref, density_ref, extra_ref, codes_out_ref, all_ref, sums_ref, codes_ref, codes_sem,
                   sems):
    span = near_ref.shape[0]
    loads = [
        pltpu.make_async_copy(ref, all_ref.at[pl.ds(i * span, span)], sems.at[i])
        for i, ref in enumerate((near_ref, even_ref, odd_ref))
    ]
    for load in loads:
        load.start()
    sums_ref[...] = sums_in_ref[...]
    for load in loads:
        load.wait()
    rows = [codes_in_ref[0:1, :], codes_in_ref[3:4, :]]
    rows += [all_ref[1 * tiles + 1, 7:8, :], all_ref[2 * tiles + 2, 7:8, :]]
    rows += [all_ref[3 * tiles + 4, 7:8, :], all_ref[6 * tiles + 5, 7:8, :]]
    for q, row in enumerate(rows):
        codes_out_ref[q : q + 1, :] = row.astype(jnp.int32)
    codes_out_ref[6:8, :] = jnp.zeros((2, codes_out_ref.shape[1]), jnp.int32)
    copy = pltpu.make_async_copy(codes_out_ref, codes_ref, codes_sem)
    copy.start()
    copy.wait()

    def one_side(target, source):
        target_block = all_ref[jnp.minimum(target, tiles - 1)]
        sums_ref[target] += density_side(all_ref[source], target_block)

    each_side(codes_ref, 6, tiles, one_side)
    lane = lax.broadcasted_iota(jnp.int32, (1, tile_size), 1)
    for t in range(tiles):
        total = jnp.sum(sums_ref[t], axis=0, keepdims=True) * (4.0 * kernel_norm)
        invalid = jnp.where(lane < counts_ref[t], 0.0, 1.0)
        scale = total + invalid
        inverse = 1.0 / scale
        density_ref[t : t + 1, :] = total
        extra_ref[t, 0:1, :] = stiff_ref[t : t + 1, :] * (total - rest_density) / (scale * scale)
        extra_ref[t, 1:2, :] = inverse


def force_self_kernel(tiles, packed_ref, extra_ref, sums_ref):
    def trip(i, carry):
        for u in range(UNROLL):
            t = i * UNROLL + u
            block = packed_ref[t]
            sums_ref[t] = force_side(block, extra_ref[t], block)
        return carry

    lax.fori_loop(0, tiles // UNROLL, trip, 0)
    sums_ref[tiles] = jnp.zeros(sums_ref.shape[1:], jnp.float32)


def force_kernel(tiles, tile_size, counts_ref, codes_ref, sums_in_ref, points_ref, speeds_ref, near_ref,
                 even_ref, odd_ref, near_extra_ref, even_extra_ref, odd_extra_ref, points_out_ref,
                 speeds_out_ref, all_ref, extra_ref, sums_ref, sems):
    span = near_ref.shape[0]
    loads = [
        pltpu.make_async_copy(ref, into.at[pl.ds(i * span, span)], sems.at[k, i])
        for k, (refs, into) in enumerate((
            ((near_ref, even_ref, odd_ref), all_ref),
            ((near_extra_ref, even_extra_ref, odd_extra_ref), extra_ref),
        ))
        for i, ref in enumerate(refs)
    ]
    for load in loads:
        load.start()
    sums_ref[...] = sums_in_ref[...]
    for load in loads:
        load.wait()

    def one_side(target, source):
        target_block = all_ref[jnp.minimum(target, tiles - 1)]
        sums_ref[target] += force_side(all_ref[source], extra_ref[source], target_block)

    each_side(codes_ref, 6, tiles, one_side)
    lane = lax.broadcasted_iota(jnp.int32, (1, tile_size), 1)
    for t in range(tiles):
        sums = sums_ref[t]
        press, inverse = extra_ref[t, 0:1, :], extra_ref[t, 1:2, :]
        valid = jnp.where(lane < counts_ref[t], 1.0, 0.0)
        for c in range(3):
            row = c * tiles + t
            half_point = all_ref[t, c : c + 1, :]
            speed = speeds_ref[row : row + 1, :]
            push = press * (sums[c : c + 1] - half_point * sums[3:4]) + (
                sums[8 + c : 9 + c] - half_point * sums[11:12]
            )
            drag = (2.0 * viscosity) * inverse * (speed * sums[7:8] - sums[4 + c : 5 + c])
            accel = (-5.0 * kernel_norm) * (2.0 * push + drag)
            new_speed = speed + time_step * valid * accel
            speeds_out_ref[row : row + 1, :] = new_speed
            points_out_ref[row : row + 1, :] = points_ref[row : row + 1, :] + time_step * new_speed


def body(positions, velocities, mass, stiffness, counts, pairs, pair_count):
    tiles = counts.shape[2]
    slot_count = positions.shape[3]
    tile_size = slot_count // tiles
    rows = pairs.shape[0]
    width_gy = lax.axis_size("gy")
    where = jnp.stack([lax.axis_index("gx"), lax.axis_index("gy")]).astype(jnp.int32)
    points = positions.reshape(3 * tiles, tile_size)
    speeds = velocities.reshape(3 * tiles, tile_size)
    counts = counts.reshape(tiles)
    smem = pl.BlockSpec(memory_space=pltpu.SMEM)
    vmem = pl.BlockSpec(memory_space=pltpu.VMEM)
    anywhere = pl.BlockSpec(memory_space=pl.ANY)
    f32 = jnp.float32

    packed, codes = pl.pallas_call(
        functools.partial(pack_kernel, tiles, tile_size, width_gy),
        out_shape=(
            jax.ShapeDtypeStruct((tiles, FIELDS, tile_size), f32),
            jax.ShapeDtypeStruct((8, rows), f32),
        ),
        in_specs=[smem, smem, smem, vmem, vmem, vmem, vmem],
        out_specs=(vmem, vmem),
        name="pack",
    )(where, counts, pair_count, points, speeds, mass.reshape(tiles, tile_size), pairs)

    def cost(sides, per_side):
        return pl.CostEstimate(
            flops=sides * per_side * tile_size * tile_size, transcendentals=0, bytes_accessed=1 << 20
        )

    along_gx = swapped(packed, "gx")
    self_sums = pl.pallas_call(
        functools.partial(density_self_kernel, tiles),
        out_shape=jax.ShapeDtypeStruct((tiles + 1, 8, tile_size), f32),
        in_specs=[vmem],
        out_specs=vmem,
        cost_estimate=cost(tiles, 20),
        name="density_self",
    )(packed)
    near = jnp.concatenate([packed] + along_gx, axis=0)
    even, odd = swapped(near, "gy")
    density, extra, codes = pl.pallas_call(
        functools.partial(density_kernel, tiles, tile_size),
        out_shape=(
            jax.ShapeDtypeStruct((tiles, tile_size), f32),
            jax.ShapeDtypeStruct((tiles, 2, tile_size), f32),
            jax.ShapeDtypeStruct((8, rows), jnp.int32),
        ),
        in_specs=[smem, vmem, vmem, vmem, anywhere, anywhere, anywhere],
        out_specs=(vmem, vmem, vmem),
        scratch_shapes=[
            pltpu.VMEM((9 * tiles, FIELDS, tile_size), f32),
            pltpu.VMEM((tiles + 1, 8, tile_size), f32),
            pltpu.SMEM((8, rows), jnp.int32),
            pltpu.SemaphoreType.DMA,
            pltpu.SemaphoreType.DMA((3,)),
        ],
        cost_estimate=cost(4 * tiles, 20),
        name="density",
    )(counts, self_sums, stiffness.reshape(tiles, tile_size), codes, near, even, odd)

    extra_gx = swapped(extra, "gx")
    self_force = pl.pallas_call(
        functools.partial(force_self_kernel, tiles),
        out_shape=jax.ShapeDtypeStruct((tiles + 1, 16, tile_size), f32),
        in_specs=[vmem, vmem],
        out_specs=vmem,
        cost_estimate=cost(tiles, 30),
        name="force_self",
    )(packed, extra)
    near_extra = jnp.concatenate([extra] + extra_gx, axis=0)
    even_extra, odd_extra = swapped(near_extra, "gy")
    new_points, new_speeds = pl.pallas_call(
        functools.partial(force_kernel, tiles, tile_size),
        out_shape=(
            jax.ShapeDtypeStruct((3 * tiles, tile_size), f32),
            jax.ShapeDtypeStruct((3 * tiles, tile_size), f32),
        ),
        in_specs=[smem, smem, vmem, vmem, vmem] + [anywhere] * 6,
        out_specs=(vmem, vmem),
        scratch_shapes=[
            pltpu.VMEM((9 * tiles, FIELDS, tile_size), f32),
            pltpu.VMEM((9 * tiles, 2, tile_size), f32),
            pltpu.VMEM((tiles + 1, 16, tile_size), f32),
            pltpu.SemaphoreType.DMA((2, 3)),
        ],
        cost_estimate=cost(4 * tiles, 30),
        name="force",
    )(counts, codes, self_force, points, speeds, near, even, odd, near_extra, even_extra, odd_extra)
    return (
        new_points.reshape(positions.shape),
        new_speeds.reshape(velocities.shape),
        density.reshape(mass.shape),
    )


def solution(mesh):
    placed = (
        P(None, "gx", "gy", None),
        P(None, "gx", "gy", None),
        P("gx", "gy", None),
        P("gx", "gy", None),
        P("gx", "gy", None),
        P(("gx", "gy"), None),
        P(("gx", "gy")),
    )
    return jax.shard_map(
        body,
        mesh=mesh,
        in_specs=placed,
        out_specs=(P(None, "gx", "gy", None), P(None, "gx", "gy", None), P("gx", "gy", None)),
        check_vma=False,
    )
```

```python
import functools
import math

import jax
import jax.numpy as jnp
from jax import lax
from jax.experimental import pallas as pl
from jax.experimental.pallas import tpu as pltpu
from jax.sharding import PartitionSpec as P

kernel_norm = 21.0 / (16.0 * math.pi)
viscosity = 0.1
time_step = 0.02
rest_density = 1.0
FIELDS = 8
UNROLL = 8


def code_shift(tiles):
    return 1 << tiles.bit_length()


def swap_routes(axis):
    count = lax.axis_size(axis)
    routes = []
    for parity in (0, 1):
        route = []
        for i in range(parity, count - 1, 2):
            route += [(i, i + 1), (i + 1, i)]
        routes.append(route)
    return routes


def swapped(block, axis):
    return [lax.ppermute(block, axis, route) for route in swap_routes(axis)]


def split_int(value, size):
    if size & (size - 1) == 0:
        return value >> (size.bit_length() - 1), value & (size - 1)
    return lax.div(value, jnp.int32(size)), lax.rem(value, jnp.int32(size))


def partner_slot(step, here):
    even = lax.rem(here, 2) == 0
    up = jnp.where(even, 1, 2)
    return jnp.where(step == 0, 0, jnp.where(step > 0, up, 3 - up))


def pack_kernel(tiles, tile_size, width_gy, where_ref, counts_ref, live_ref, points_ref, speeds_ref,
                mass_ref, pairs_ref, packed_ref, codes_ref):
    rows = pairs_ref.shape[0]
    shift = code_shift(tiles)
    row_here, column_here = where_ref[0], where_ref[1]
    lane = lax.broadcasted_iota(jnp.int32, (1, tile_size), 1)
    for t in range(tiles):
        for c in range(3):
            packed_ref[t, c : c + 1, :] = 0.5 * points_ref[c * tiles + t : c * tiles + t + 1, :] - 0.5
            packed_ref[t, 4 + c : 5 + c, :] = speeds_ref[c * tiles + t : c * tiles + t + 1, :]
        packed_ref[t, 3:4, :] = jnp.where(lane < counts_ref[t], mass_ref[t : t + 1, :], 0.0)
        packed_ref[t, 7:8, :] = jnp.zeros((1, tile_size), jnp.float32)
    box, slot = split_int(pairs_ref[...], tiles)
    box_gx, box_gy = split_int(box, width_gy)
    side_a = partner_slot(box_gx[:, 0:1] - row_here, row_here)
    side_b = partner_slot(box_gy[:, 1:2] - column_here, column_here)
    slot_a, slot_b = slot[:, 0:1], slot[:, 1:2]
    row_index = lax.broadcasted_iota(jnp.int32, (rows, 1), 0)
    live = (row_index >= tiles) & (row_index < live_ref[0])
    cross = live & (pairs_ref[:, 0:1] != pairs_ref[:, 1:2])
    group_a = jnp.where(live, side_a, 7)
    group_b = jnp.where(cross, side_b + 3, 7)
    source_box = (side_b * 3 + side_a) * tiles
    code_a = (slot_a + shift * (source_box + slot_b)).astype(jnp.float32)
    code_b = (slot_b + shift * (source_box + slot_a)).astype(jnp.float32)
    lanes = lax.broadcasted_iota(jnp.int32, (rows, rows), 1)
    subs = lax.broadcasted_iota(jnp.int32, (rows, rows), 0)
    flags = jnp.where((lanes == group_a) | (lanes == group_b), 1.0, 0.0)
    flags = jnp.where(lanes < 6, flags, 0.0)
    below = jnp.where(lanes < subs, 1.0, 0.0).astype(jnp.bfloat16)
    places = jnp.dot(below, flags.astype(jnp.bfloat16), preferred_element_type=jnp.float32)
    totals = jnp.sum(flags, axis=0, keepdims=True)
    codes_ref[...] = jnp.zeros(codes_ref.shape, jnp.float32)
    for q in range(6):
        group, code = (group_a, code_a) if q < 3 else (group_b, code_b)
        place = jnp.where(group == q, places[:, q : q + 1].astype(jnp.int32), -1)
        listed = jnp.sum(jnp.where(place == lanes, code, 0.0), axis=0, keepdims=True)
        total = totals[:, q : q + 1]
        row_lane = lanes[0:1, :]
        listed = jnp.where(row_lane < total.astype(jnp.int32), listed, float(tiles))
        listed = jnp.where(row_lane == rows - 1, total, listed)
        codes_ref[q : q + 1, :] = listed
        if q not in (0, 3):
            packed_ref[q, 7:8, :] = listed


def split_terms(values, terms):
    parts = []
    rest = values
    for i in range(terms):
        part = rest.astype(jnp.bfloat16)
        parts.append(part)
        if i + 1 < terms:
            rest = rest - part.astype(jnp.float32)
    return parts


def point_terms(block):
    sub = lax.broadcasted_iota(jnp.int32, block.shape, 0)
    points = jnp.where(sub < 3, block, 0.0)
    first, second = [part.astype(jnp.float32) for part in split_terms(points, 2)]
    kept = first + second
    length = jnp.sum(kept * kept, axis=0, keepdims=True)
    rest = jnp.where(sub < 6, length, block[3:4, :])
    q1, q2, q3 = [part.astype(jnp.float32) for part in split_terms(rest, 3)]
    return sub, first, second, q1, q2, q3


def source_terms(block):
    sub, first, second, q1, q2, q3 = point_terms(block)
    top = jnp.where((sub == 3) | (sub == 6), q1, jnp.where(sub == 5, q3, q2))
    top = jnp.where(sub < 3, first, top)
    ones = jnp.where(sub < 3, first, jnp.where(sub == 6, q3, jnp.where(sub < 6, 1.0, 0.0)))
    return jnp.concatenate([top, ones, second, second], axis=0).T


def target_terms(block):
    sub, first, second, q1, q2, q3 = point_terms(block)
    first, second = -2.0 * first, -2.0 * second
    top = jnp.where(sub < 3, first, jnp.where(sub < 6, 1.0, 0.0))
    lengths = jnp.where(sub == 3, q1, jnp.where(sub == 4, q2, jnp.where(sub == 5, q3, second)))
    return jnp.concatenate([top, lengths, first, second], axis=0)


def mass_picks(tile_size):
    row = lax.broadcasted_iota(jnp.int32, (4 * FIELDS, tile_size), 0)
    return jnp.where((row == 6) | (row == 7) | (row == FIELDS + 6), 1.0, 0.0)


def falloff_of(square):
    square = jnp.maximum(square, 1e-24)
    return jnp.maximum(1.0 - square * lax.rsqrt(square), 0.0)


def density_side(source_block, targets, picks):
    size = source_block.shape[1]
    both = jnp.dot(
        source_terms(source_block),
        jnp.concatenate([targets, picks], axis=1),
        preferred_element_type=jnp.float32,
    )
    total = None
    for j in range(0, size, 8):
        falloff = falloff_of(both[j : j + 8, 0:size])
        f2 = falloff * falloff
        term = f2 * f2 * ((1.25 - falloff) * both[j : j + 8, size:])
        total = term if total is None else total + term
    return total


def force_side(source_block, source_extra, targets):
    size = source_block.shape[1]
    squares = jnp.dot(source_terms(source_block), targets, preferred_element_type=jnp.float32)
    high, low = [], []
    for j in range(0, size, 16):
        falloff = falloff_of(squares[j : j + 16])
        top, rest = split_terms(falloff * falloff * falloff, 2)
        high.append(top)
        low.append(rest)
    slope = jnp.concatenate(high + low, axis=0)
    sub = lax.broadcasted_iota(jnp.int32, source_block.shape, 0)
    base = jnp.where((sub == 3) | (sub == 7), 1.0, source_block)
    mass = source_block[3:4, :]
    mass_press = mass * source_extra[0:1, :]
    mass_inverse = mass * source_extra[1:2, :]
    columns = jnp.concatenate(
        [base * jnp.where(sub < 4, mass, mass_inverse), base * mass_press], axis=0
    )
    columns = jnp.concatenate(split_terms(columns, 3), axis=0)
    columns = jnp.concatenate([columns, columns], axis=1)
    sums = jnp.dot(columns, slope, preferred_element_type=jnp.float32)
    return sums[0:16] + sums[16:32] + sums[32:48]


def merge_lists(lists_ref, merged_ref, lists, dummy):
    last = lists_ref.shape[1] - 1

    def over_list(q, start):
        count = lists_ref[q, last]

        def chunk(i, carry):
            for k in range(8):
                merged_ref[start + 8 * i + k] = lists_ref[q, 8 * i + k]
            return carry

        lax.fori_loop(0, (count + 7) // 8, chunk, 0)
        return start + count

    total = lax.fori_loop(0, lists, over_list, 0)
    for k in range(UNROLL):
        merged_ref[total + k] = dummy
    merged_ref[merged_ref.shape[0] - 1] = total


def each_side(merged_ref, tiles, one_side):
    shift = code_shift(tiles)
    trips = (merged_ref[merged_ref.shape[0] - 1] + UNROLL - 1) // UNROLL

    def trip(i, carry):
        for u in range(UNROLL):
            code = merged_ref[i * UNROLL + u]
            one_side(code & (shift - 1), code >> (shift.bit_length() - 1))
        return carry

    lax.fori_loop(0, trips, trip, 0)


def density_self_kernel(tiles, packed_ref, sums_ref):
    picks = mass_picks(packed_ref.shape[2])

    def trip(i, carry):
        for u in range(UNROLL):
            t = i * UNROLL + u
            block = packed_ref[t]
            sums_ref[t] = density_side(block, target_terms(block), picks)
        return carry

    lax.fori_loop(0, tiles // UNROLL, trip, 0)
    sums_ref[tiles] = jnp.zeros(sums_ref.shape[1:], jnp.float32)


def fill_targets(tiles, blocks_ref, targets_ref):
    def trip(i, carry):
        for u in range(UNROLL):
            t = i * UNROLL + u
            targets_ref[t] = target_terms(blocks_ref[t])
        return carry

    lax.fori_loop(0, tiles // UNROLL, trip, 0)
    targets_ref[tiles] = jnp.zeros(targets_ref.shape[1:], jnp.float32)


def density_kernel(tiles, tile_size, counts_ref, sums_in_ref, stiff_ref, codes_in_ref, packed_ref, near_ref,
                   even_ref, odd_ref, density_ref, extra_ref, merged_ref, all_ref, sums_ref, targets_ref,
                   lists_ref, codes_ref, codes_sem, sems):
    span = near_ref.shape[0]
    loads = [
        pltpu.make_async_copy(ref, all_ref.at[pl.ds(i * span, span)], sems.at[i])
        for i, ref in enumerate((near_ref, even_ref, odd_ref))
    ]
    for load in loads:
        load.start()
    sums_ref[...] = sums_in_ref[...]
    fill_targets(tiles, packed_ref, targets_ref)
    for load in loads:
        load.wait()
    rows = [codes_in_ref[0:1, :], codes_in_ref[3:4, :]]
    rows += [all_ref[1 * tiles + 1, 7:8, :], all_ref[2 * tiles + 2, 7:8, :]]
    rows += [all_ref[3 * tiles + 4, 7:8, :], all_ref[6 * tiles + 5, 7:8, :]]
    for q, row in enumerate(rows):
        lists_ref[q : q + 1, :] = row.astype(jnp.int32)
    lists_ref[6:8, :] = jnp.zeros((2, lists_ref.shape[1]), jnp.int32)
    copy = pltpu.make_async_copy(lists_ref, codes_ref, codes_sem)
    copy.start()
    copy.wait()
    merge_lists(codes_ref, merged_ref, 6, tiles)
    picks = mass_picks(tile_size)

    def one_side(target, source):
        sums_ref[target] += density_side(all_ref[source], targets_ref[target], picks)

    each_side(merged_ref, tiles, one_side)
    lane = lax.broadcasted_iota(jnp.int32, (1, tile_size), 1)
    for t in range(tiles):
        total = jnp.sum(sums_ref[t], axis=0, keepdims=True) * (4.0 * kernel_norm)
        invalid = jnp.where(lane < counts_ref[t], 0.0, 1.0)
        scale = total + invalid
        inverse = 1.0 / scale
        density_ref[t : t + 1, :] = total
        extra_ref[t, 0:1, :] = stiff_ref[t : t + 1, :] * (total - rest_density) / (scale * scale)
        extra_ref[t, 1:2, :] = inverse


def force_self_kernel(tiles, packed_ref, extra_ref, sums_ref):
    def trip(i, carry):
        for u in range(UNROLL):
            t = i * UNROLL + u
            block = packed_ref[t]
            sums_ref[t] = force_side(block, extra_ref[t], target_terms(block))
        return carry

    lax.fori_loop(0, tiles // UNROLL, trip, 0)
    sums_ref[tiles] = jnp.zeros(sums_ref.shape[1:], jnp.float32)


def force_kernel(tiles, tile_size, counts_ref, merged_ref, sums_in_ref, points_ref, speeds_ref, packed_ref, near_ref,
                 even_ref, odd_ref, near_extra_ref, even_extra_ref, odd_extra_ref, points_out_ref,
                 speeds_out_ref, all_ref, extra_ref, sums_ref, targets_ref, sems):
    span = near_ref.shape[0]
    loads = [
        pltpu.make_async_copy(ref, into.at[pl.ds(i * span, span)], sems.at[k, i])
        for k, (refs, into) in enumerate((
            ((near_ref, even_ref, odd_ref), all_ref),
            ((near_extra_ref, even_extra_ref, odd_extra_ref), extra_ref),
        ))
        for i, ref in enumerate(refs)
    ]
    for load in loads:
        load.start()
    sums_ref[...] = sums_in_ref[...]
    fill_targets(tiles, packed_ref, targets_ref)
    for load in loads:
        load.wait()

    def one_side(target, source):
        sums_ref[target] += force_side(all_ref[source], extra_ref[source], targets_ref[target])

    each_side(merged_ref, tiles, one_side)
    lane = lax.broadcasted_iota(jnp.int32, (1, tile_size), 1)
    for t in range(tiles):
        sums = sums_ref[t]
        press, inverse = extra_ref[t, 0:1, :], extra_ref[t, 1:2, :]
        valid = jnp.where(lane < counts_ref[t], 1.0, 0.0)
        for c in range(3):
            row = c * tiles + t
            half_point = all_ref[t, c : c + 1, :]
            speed = speeds_ref[row : row + 1, :]
            push = press * (sums[c : c + 1] - half_point * sums[3:4]) + (
                sums[8 + c : 9 + c] - half_point * sums[11:12]
            )
            drag = (2.0 * viscosity) * inverse * (speed * sums[7:8] - sums[4 + c : 5 + c])
            accel = (-5.0 * kernel_norm) * (2.0 * push + drag)
            new_speed = speed + time_step * valid * accel
            speeds_out_ref[row : row + 1, :] = new_speed
            points_out_ref[row : row + 1, :] = points_ref[row : row + 1, :] + time_step * new_speed


def body(positions, velocities, mass, stiffness, counts, pairs, pair_count):
    tiles = counts.shape[2]
    slot_count = positions.shape[3]
    tile_size = slot_count // tiles
    rows = pairs.shape[0]
    width_gy = lax.axis_size("gy")
    where = jnp.stack([lax.axis_index("gx"), lax.axis_index("gy")]).astype(jnp.int32)
    points = positions.reshape(3 * tiles, tile_size)
    speeds = velocities.reshape(3 * tiles, tile_size)
    counts = counts.reshape(tiles)
    smem = pl.BlockSpec(memory_space=pltpu.SMEM)
    vmem = pl.BlockSpec(memory_space=pltpu.VMEM)
    anywhere = pl.BlockSpec(memory_space=pl.ANY)
    f32 = jnp.float32

    packed, codes = pl.pallas_call(
        functools.partial(pack_kernel, tiles, tile_size, width_gy),
        out_shape=(
            jax.ShapeDtypeStruct((tiles, FIELDS, tile_size), f32),
            jax.ShapeDtypeStruct((8, rows), f32),
        ),
        in_specs=[smem, smem, smem, vmem, vmem, vmem, vmem],
        out_specs=(vmem, vmem),
        name="pack",
    )(where, counts, pair_count, points, speeds, mass.reshape(tiles, tile_size), pairs)

    def cost(sides, per_side):
        return pl.CostEstimate(
            flops=sides * per_side * tile_size * tile_size, transcendentals=0, bytes_accessed=1 << 20
        )

    along_gx = swapped(packed, "gx")
    self_sums = pl.pallas_call(
        functools.partial(density_self_kernel, tiles),
        out_shape=jax.ShapeDtypeStruct((tiles + 1, 8, tile_size), f32),
        in_specs=[vmem],
        out_specs=vmem,
        cost_estimate=cost(tiles, 20),
        name="density_self",
    )(packed)
    near = jnp.concatenate([packed] + along_gx, axis=0)
    even, odd = swapped(near, "gy")
    density, extra, merged = pl.pallas_call(
        functools.partial(density_kernel, tiles, tile_size),
        out_shape=(
            jax.ShapeDtypeStruct((tiles, tile_size), f32),
            jax.ShapeDtypeStruct((tiles, 2, tile_size), f32),
            jax.ShapeDtypeStruct((8 * rows,), jnp.int32),
        ),
        in_specs=[smem, vmem, vmem, vmem, vmem, anywhere, anywhere, anywhere],
        out_specs=(vmem, vmem, smem),
        scratch_shapes=[
            pltpu.VMEM((9 * tiles, FIELDS, tile_size), f32),
            pltpu.VMEM((tiles + 1, 8, tile_size), f32),
            pltpu.VMEM((tiles + 1, 4 * FIELDS, tile_size), f32),
            pltpu.VMEM((8, rows), jnp.int32),
            pltpu.SMEM((8, rows), jnp.int32),
            pltpu.SemaphoreType.DMA,
            pltpu.SemaphoreType.DMA((3,)),
        ],
        cost_estimate=cost(4 * tiles, 20),
        name="density",
    )(counts, self_sums, stiffness.reshape(tiles, tile_size), codes, packed, near, even, odd)

    extra_gx = swapped(extra, "gx")
    self_force = pl.pallas_call(
        functools.partial(force_self_kernel, tiles),
        out_shape=jax.ShapeDtypeStruct((tiles + 1, 16, tile_size), f32),
        in_specs=[vmem, vmem],
        out_specs=vmem,
        cost_estimate=cost(tiles, 30),
        name="force_self",
    )(packed, extra)
    near_extra = jnp.concatenate([extra] + extra_gx, axis=0)
    even_extra, odd_extra = swapped(near_extra, "gy")
    new_points, new_speeds = pl.pallas_call(
        functools.partial(force_kernel, tiles, tile_size),
        out_shape=(
            jax.ShapeDtypeStruct((3 * tiles, tile_size), f32),
            jax.ShapeDtypeStruct((3 * tiles, tile_size), f32),
        ),
        in_specs=[smem, smem, vmem, vmem, vmem, vmem] + [anywhere] * 6,
        out_specs=(vmem, vmem),
        scratch_shapes=[
            pltpu.VMEM((9 * tiles, FIELDS, tile_size), f32),
            pltpu.VMEM((9 * tiles, 2, tile_size), f32),
            pltpu.VMEM((tiles + 1, 16, tile_size), f32),
            pltpu.VMEM((tiles + 1, 4 * FIELDS, tile_size), f32),
            pltpu.SemaphoreType.DMA((2, 3)),
        ],
        cost_estimate=cost(4 * tiles, 30),
        name="force",
    )(counts, merged, self_force, points, speeds, packed, near, even, odd, near_extra, even_extra, odd_extra)
    return (
        new_points.reshape(positions.shape),
        new_speeds.reshape(velocities.shape),
        density.reshape(mass.shape),
    )


def solution(mesh):
    placed = (
        P(None, "gx", "gy", None),
        P(None, "gx", "gy", None),
        P("gx", "gy", None),
        P("gx", "gy", None),
        P("gx", "gy", None),
        P(("gx", "gy"), None),
        P(("gx", "gy")),
    )
    return jax.shard_map(
        body,
        mesh=mesh,
        in_specs=placed,
        out_specs=(P(None, "gx", "gy", None), P(None, "gx", "gy", None), P("gx", "gy", None)),
        check_vma=False,
    )
```

```python
import functools
import math

import jax
import jax.numpy as jnp
from jax import lax
from jax.experimental import pallas as pl
from jax.experimental.pallas import tpu as pltpu
from jax.sharding import PartitionSpec as P

kernel_norm = 21.0 / (16.0 * math.pi)
viscosity = 0.1
time_step = 0.02
rest_density = 1.0
FIELDS = 4
UNROLL = 8
SENT = (1, 2, 4, 5)


def code_shift(tiles):
    return 1 << tiles.bit_length()


def swap_routes(axis):
    count = lax.axis_size(axis)
    routes = []
    for parity in (0, 1):
        route = []
        for i in range(parity, count - 1, 2):
            route += [(i, i + 1), (i + 1, i)]
        routes.append(route)
    return routes


def swapped(block, axis):
    return [lax.ppermute(block, axis, route) for route in swap_routes(axis)]


def split_int(value, size):
    if size & (size - 1) == 0:
        return value >> (size.bit_length() - 1), value & (size - 1)
    return lax.div(value, jnp.int32(size)), lax.rem(value, jnp.int32(size))


def partner_slot(step, here):
    even = lax.rem(here, 2) == 0
    up = jnp.where(even, 1, 2)
    return jnp.where(step == 0, 0, jnp.where(step > 0, up, 3 - up))


def fetch(sources, targets, sems):
    copies = [pltpu.make_async_copy(a, b, sems.at[i]) for i, (a, b) in enumerate(zip(sources, targets))]
    for copy in copies:
        copy.start()
    for copy in copies:
        copy.wait()


def pack_kernel(tiles, tile_size, width_gy, live_ref, counts_hbm, points_hbm, mass_hbm, pairs_hbm,
                packed_ref, codes_ref, counts_ref, points_ref, mass_ref, pairs_ref, sems):
    fetch(
        (counts_hbm, points_hbm, mass_hbm, pairs_hbm), (counts_ref, points_ref, mass_ref, pairs_ref), sems
    )
    rows = pairs_ref.shape[1]
    shift = code_shift(tiles)
    row_here, column_here = lax.axis_index("gx"), lax.axis_index("gy")
    lane = lax.broadcasted_iota(jnp.int32, (1, tile_size), 1)
    for t in range(tiles):
        for c in range(3):
            packed_ref[t, c : c + 1, :] = 0.5 * points_ref[c * tiles + t : c * tiles + t + 1, :] - 0.5
        packed_ref[t, 3:4, :] = jnp.where(lane < counts_ref[t], mass_ref[t : t + 1, :], 0.0)
    box, slot = split_int(pairs_ref[...], tiles)
    box_gx, box_gy = split_int(box, width_gy)
    side_a = partner_slot(box_gx[0:1] - row_here, row_here)
    side_b = partner_slot(box_gy[1:2] - column_here, column_here)
    slot_a, slot_b = slot[0:1], slot[1:2]
    row_index = lax.broadcasted_iota(jnp.int32, (1, rows), 1)
    live = (row_index >= tiles) & (row_index < live_ref[0])
    cross = live & (pairs_ref[0:1] != pairs_ref[1:2])
    group_a = jnp.where(live, side_a, 7)
    group_b = jnp.where(cross, side_b + 3, 7)
    source_box = (side_b * 4 + side_a) * tiles
    code_a = (slot_a + shift * (source_box + slot_b)).astype(jnp.float32)
    code_b = (slot_b + shift * (source_box + slot_a)).astype(jnp.float32)
    sub = lax.broadcasted_iota(jnp.int32, (8, rows), 0)
    listed = (sub == group_a) | (sub == group_b)
    listed = listed & (sub < 6)
    flags = jnp.where(listed, 1.0, 0.0)
    lanes = lax.broadcasted_iota(jnp.int32, (rows, rows), 1)
    subs = lax.broadcasted_iota(jnp.int32, (rows, rows), 0)
    above = jnp.where(subs < lanes, 1.0, 0.0).astype(jnp.bfloat16)
    places = jnp.dot(flags.astype(jnp.bfloat16), above, preferred_element_type=jnp.float32)
    totals = jnp.sum(flags, axis=1, keepdims=True)
    columns = jnp.where(listed, places, -1.0).T
    codes = jnp.concatenate(split_terms(jnp.where(sub < 3, code_a, code_b), 2), axis=0)
    picked = lax.broadcasted_iota(jnp.int32, (8, 8 * rows), 0)
    picks = jnp.where(picked == lax.broadcasted_iota(jnp.int32, (8, 8 * rows), 1) // rows, 1.0, 0.0)
    spread = jnp.dot(columns, picks[:, : 6 * rows], preferred_element_type=jnp.float32)
    lanes = lanes.astype(jnp.float32)
    hits = jnp.concatenate(
        [
            jnp.where(spread[:, q * rows : (q + 1) * rows] == lanes, 1.0, 0.0).astype(jnp.bfloat16)
            for q in range(6)
        ],
        axis=1,
    )
    found = jnp.dot(codes, hits, preferred_element_type=jnp.float32)
    row_lane = lanes[0:1, :]
    codes_ref[...] = jnp.zeros(codes_ref.shape, jnp.int32)
    for q in range(6):
        here = slice(q * rows, (q + 1) * rows)
        code = found[q : q + 1, here] + found[8 + q : 9 + q, here]
        total = totals[q : q + 1, :]
        code = jnp.where(row_lane < total, code, float(tiles))
        code = jnp.where(row_lane == rows - 1, total, code)
        codes_ref[q : q + 1, :] = code.astype(jnp.int32)
        if q in SENT:
            place = SENT.index(q)
            packed_ref[tiles, place : place + 1, :] = code


def split_terms(values, terms):
    parts = []
    rest = values
    for i in range(terms):
        part = rest.astype(jnp.bfloat16)
        parts.append(part)
        if i + 1 < terms:
            rest = rest - part.astype(jnp.float32)
    return parts


def point_terms(block):
    block = jnp.concatenate([block, block], axis=0)
    sub = lax.broadcasted_iota(jnp.int32, block.shape, 0)
    points = jnp.where(sub < 3, block, 0.0)
    first, second = [part.astype(jnp.float32) for part in split_terms(points, 2)]
    kept = first + second
    length = jnp.sum(kept * kept, axis=0, keepdims=True)
    rest = jnp.where(sub < 6, length, block[3:4, :])
    q1, q2, q3 = [part.astype(jnp.float32) for part in split_terms(rest, 3)]
    return sub, first, second, q1, q2, q3


def source_terms(block):
    sub, first, second, q1, q2, q3 = point_terms(block)
    top = jnp.where((sub == 3) | (sub == 6), q1, jnp.where(sub == 5, q3, q2))
    top = jnp.where(sub < 3, first, top)
    ones = jnp.where(sub < 3, first, jnp.where(sub == 6, q3, jnp.where(sub < 6, 1.0, 0.0)))
    return jnp.concatenate([top, ones, second, second], axis=0).T


def target_terms(block):
    sub, first, second, q1, q2, q3 = point_terms(block)
    first, second = -2.0 * first, -2.0 * second
    top = jnp.where(sub < 3, first, jnp.where(sub < 6, 1.0, 0.0))
    lengths = jnp.where(sub == 3, q1, jnp.where(sub == 4, q2, jnp.where(sub == 5, q3, second)))
    return jnp.concatenate([top, lengths, first, second], axis=0)


def mass_picks(tile_size):
    row = lax.broadcasted_iota(jnp.int32, (32, tile_size), 0)
    return jnp.where((row == 6) | (row == 7) | (row == 14), 1.0, 0.0)


def falloff_of(square):
    square = jnp.maximum(square, 1e-24)
    return jnp.maximum(1.0 - square * lax.rsqrt(square), 0.0)


def density_side(source_block, targets, picks):
    size = source_block.shape[1]
    both = jnp.dot(
        source_terms(source_block),
        jnp.concatenate([targets, picks], axis=1),
        preferred_element_type=jnp.float32,
    )
    total = None
    for j in range(0, size, 8):
        falloff = falloff_of(both[j : j + 8, 0:size])
        f2 = falloff * falloff
        term = f2 * f2 * ((1.25 - falloff) * both[j : j + 8, size:])
        total = term if total is None else total + term
    return total


def force_side(source_block, extra_block, last_speed, targets):
    size = source_block.shape[1]
    squares = jnp.dot(source_terms(source_block), targets, preferred_element_type=jnp.float32)
    high, low = [], []
    for j in range(0, size, 16):
        falloff = falloff_of(squares[j : j + 16])
        top, rest = split_terms(falloff * falloff * falloff, 2)
        high.append(top)
        low.append(rest)
    slope = jnp.concatenate(high + low, axis=0)
    base = jnp.concatenate([source_block, extra_block], axis=0)
    sub = lax.broadcasted_iota(jnp.int32, base.shape, 0)
    base = jnp.where((sub == 3) | (sub == 7), 1.0, jnp.where(sub == 6, last_speed, base))
    mass = source_block[3:4, :]
    mass_press = mass * extra_block[2:3, :]
    mass_inverse = mass * extra_block[3:4, :]
    columns = jnp.concatenate(
        [base * jnp.where(sub < 4, mass, mass_inverse), base * mass_press], axis=0
    )
    columns = jnp.concatenate(split_terms(columns, 3), axis=0)
    columns = jnp.concatenate([columns, columns], axis=1)
    sums = jnp.dot(columns, slope, preferred_element_type=jnp.float32)
    return sums[0:16] + sums[16:32] + sums[32:48]


def merge_lists(lists_ref, merged_ref, lists, dummy):
    last = lists_ref.shape[1] - 1

    def over_list(q, start):
        count = lists_ref[q, last]

        def chunk(i, carry):
            for k in range(8):
                merged_ref[start + 8 * i + k] = lists_ref[q, 8 * i + k]
            return carry

        lax.fori_loop(0, (count + 7) // 8, chunk, 0)
        return start + count

    total = lax.fori_loop(0, lists, over_list, 0)
    for k in range(UNROLL):
        merged_ref[total + k] = dummy
    merged_ref[merged_ref.shape[0] - 1] = total


def each_side(count, code_at, tiles, one_side):
    shift = code_shift(tiles)

    def trip(i, carry):
        for u in range(UNROLL):
            code = code_at(i * UNROLL + u)
            one_side(code & (shift - 1), code >> (shift.bit_length() - 1))
        return carry

    lax.fori_loop(0, (count + UNROLL - 1) // UNROLL, trip, 0)


def merged_sides(merged_ref, tiles, one_side):
    count = merged_ref[merged_ref.shape[0] - 1]
    each_side(count, lambda k: merged_ref[k], tiles, one_side)


def own_sides(codes_ref, tiles, one_side):
    count = codes_ref[3, codes_ref.shape[1] - 1]
    each_side(count, lambda k: codes_ref[3, k], tiles, one_side)


def each_tile(tiles, one_tile):
    def trip(i, carry):
        for u in range(UNROLL):
            one_tile(i * UNROLL + u)
        return carry

    lax.fori_loop(0, tiles // UNROLL, trip, 0)


def density_self_kernel(tiles, packed_ref, sums_ref, targets_ref):
    picks = mass_picks(packed_ref.shape[2])

    def one_tile(t):
        block = packed_ref[t]
        targets = target_terms(block)
        targets_ref[t] = targets
        sums_ref[t] = density_side(block, targets, picks)

    each_tile(tiles, one_tile)
    sums_ref[tiles] = jnp.zeros(sums_ref.shape[1:], jnp.float32)
    targets_ref[tiles] = jnp.zeros(targets_ref.shape[1:], jnp.float32)


def take(refs, source, tiles, extra_rows):
    box, slot = split_int(source, tiles)
    place = (box & 3) * (tiles + extra_rows) + slot
    blocks = [ref[place] for ref in refs]
    if len(refs) == 1:
        return blocks[0]
    return jnp.where(box < 4, blocks[0], jnp.where(box < 8, blocks[1], blocks[2]))


def take_speed(refs, source, tiles, extra_rows):
    box, slot = split_int(source, tiles)
    place = (box & 3) * (tiles + extra_rows) + tiles + (slot >> 2)
    rows = [ref[place, pl.ds(slot & 3, 1), :] for ref in refs]
    if len(refs) == 1:
        return rows[0]
    return jnp.where(box < 4, rows[0], jnp.where(box < 8, rows[1], rows[2]))


def density_near_kernel(tiles, codes_in_ref, sums_in_ref, targets_ref, near_ref, sums_ref, codes_ref, sem):
    copy = pltpu.make_async_copy(codes_in_ref, codes_ref, sem)
    copy.start()
    sums_ref[...] = sums_in_ref[...]
    copy.wait()
    picks = mass_picks(near_ref.shape[2])

    def one_side(target, source):
        block = take((near_ref,), source, tiles, 1)
        sums_ref[target] += density_side(block, targets_ref[target], picks)

    own_sides(codes_ref, tiles, one_side)


def density_kernel(tiles, tile_size, counts_hbm, sums_in_ref, targets_ref, stiff_ref, speeds_ref, codes_in_ref,
                   near_ref, even_ref, odd_ref, density_ref, extra_ref, merged_ref, sums_ref, lists_ref,
                   codes_ref, counts_ref, sems):
    rows = [codes_in_ref[0:1, :].astype(jnp.float32)]
    rows += [near_ref[g * (tiles + 1) + tiles, g - 1 : g, :] for g in (1, 2)]
    rows += [even_ref[tiles, 2:3, :], odd_ref[tiles, 3:4, :]]
    for q, row in enumerate(rows):
        lists_ref[q : q + 1, :] = row.astype(jnp.int32)
    lists_ref[5:8, :] = jnp.zeros((3, lists_ref.shape[1]), jnp.int32)
    copy = pltpu.make_async_copy(lists_ref, codes_ref, sems.at[0])
    copy.start()
    counts_copy = pltpu.make_async_copy(counts_hbm, counts_ref, sems.at[1])
    counts_copy.start()
    sums_ref[...] = sums_in_ref[...]
    for t in range(tiles):
        for c in range(2):
            extra_ref[t, c : c + 1, :] = speeds_ref[c * tiles + t : c * tiles + t + 1, :]
        extra_ref[tiles + t // 4, t % 4 : t % 4 + 1, :] = speeds_ref[2 * tiles + t : 2 * tiles + t + 1, :]
    copy.wait()
    merge_lists(codes_ref, merged_ref, 5, tiles)
    picks = mass_picks(tile_size)

    def one_side(target, source):
        block = take((near_ref, even_ref, odd_ref), source, tiles, 1)
        sums_ref[target] += density_side(block, targets_ref[target], picks)

    merged_sides(merged_ref, tiles, one_side)
    counts_copy.wait()
    lane = lax.broadcasted_iota(jnp.int32, (1, tile_size), 1)
    for t in range(tiles):
        total = jnp.sum(sums_ref[t], axis=0, keepdims=True) * (4.0 * kernel_norm)
        invalid = jnp.where(lane < counts_ref[t], 0.0, 1.0)
        scale = total + invalid
        inverse = 1.0 / scale
        density_ref[t : t + 1, :] = total
        extra_ref[t, 2:3, :] = stiff_ref[t : t + 1, :] * (total - rest_density) / (scale * scale)
        extra_ref[t, 3:4, :] = inverse


def force_self_kernel(tiles, packed_ref, targets_ref, extra_ref, sums_ref):
    def one_tile(t):
        last_speed = take_speed((extra_ref,), t, tiles, tiles // 4)
        sums_ref[t] = force_side(packed_ref[t], extra_ref[t], last_speed, targets_ref[t])

    each_tile(tiles, one_tile)
    sums_ref[tiles] = jnp.zeros(sums_ref.shape[1:], jnp.float32)


def force_near_kernel(tiles, codes_in_ref, sums_in_ref, targets_ref, near_ref, near_extra_ref, sums_ref,
                      codes_ref, sem):
    copy = pltpu.make_async_copy(codes_in_ref, codes_ref, sem)
    copy.start()
    sums_ref[...] = sums_in_ref[...]
    copy.wait()

    def one_side(target, source):
        block = take((near_ref,), source, tiles, 1)
        extra = take((near_extra_ref,), source, tiles, tiles // 4)
        last_speed = take_speed((near_extra_ref,), source, tiles, tiles // 4)
        sums_ref[target] += force_side(block, extra, last_speed, targets_ref[target])

    own_sides(codes_ref, tiles, one_side)


def force_kernel(tiles, tile_size, counts_hbm, merged_ref, sums_in_ref, targets_ref, points_ref, speeds_ref,
                 near_ref, even_ref, odd_ref, near_extra_ref, even_extra_ref, odd_extra_ref, points_out_ref,
                 speeds_out_ref, sums_ref, counts_ref, sem):
    counts_copy = pltpu.make_async_copy(counts_hbm, counts_ref, sem)
    counts_copy.start()
    sums_ref[...] = sums_in_ref[...]

    def one_side(target, source):
        extras = (near_extra_ref, even_extra_ref, odd_extra_ref)
        block = take((near_ref, even_ref, odd_ref), source, tiles, 1)
        extra = take(extras, source, tiles, tiles // 4)
        last_speed = take_speed(extras, source, tiles, tiles // 4)
        sums_ref[target] += force_side(block, extra, last_speed, targets_ref[target])

    merged_sides(merged_ref, tiles, one_side)
    counts_copy.wait()
    lane = lax.broadcasted_iota(jnp.int32, (1, tile_size), 1)
    for t in range(tiles):
        sums = sums_ref[t]
        press, inverse = near_extra_ref[t, 2:3, :], near_extra_ref[t, 3:4, :]
        valid = jnp.where(lane < counts_ref[t], 1.0, 0.0)
        for c in range(3):
            row = c * tiles + t
            half_point = near_ref[t, c : c + 1, :]
            speed = speeds_ref[row : row + 1, :]
            push = press * (sums[c : c + 1] - half_point * sums[3:4]) + (
                sums[8 + c : 9 + c] - half_point * sums[11:12]
            )
            drag = (2.0 * viscosity) * inverse * (speed * sums[7:8] - sums[4 + c : 5 + c])
            accel = (-5.0 * kernel_norm) * (2.0 * push + drag)
            new_speed = speed + time_step * valid * accel
            speeds_out_ref[row : row + 1, :] = new_speed
            points_out_ref[row : row + 1, :] = points_ref[row : row + 1, :] + time_step * new_speed


def body(positions, velocities, mass, stiffness, counts, pairs, pair_count):
    tiles = counts.shape[2]
    slot_count = positions.shape[3]
    tile_size = slot_count // tiles
    rows = pairs.shape[0]
    width_gy = lax.axis_size("gy")
    points = positions.reshape(3 * tiles, tile_size)
    speeds = velocities.reshape(3 * tiles, tile_size)
    counts = counts.reshape(tiles)
    smem = pl.BlockSpec(memory_space=pltpu.SMEM)
    vmem = pl.BlockSpec(memory_space=pltpu.VMEM)
    hbm = pl.BlockSpec(memory_space=pltpu.HBM)
    f32 = jnp.float32

    def call(kernel, name, outs, ins, scratch, sides=0):
        params = dict(cost_estimate=pl.CostEstimate(
            flops=sides * 25 * tile_size * tile_size, transcendentals=0, bytes_accessed=1 << 20
        ))
        return pl.pallas_call(
            kernel,
            out_shape=tuple(out for out, _ in outs),
            in_specs=ins,
            out_specs=tuple(space for _, space in outs),
            scratch_shapes=scratch,
            compiler_params=pltpu.CompilerParams(vmem_limit_bytes=12 << 20),
            name=name,
            **params,
        )

    def array(*shape, dtype=f32):
        return jax.ShapeDtypeStruct(shape, dtype)

    dma = pltpu.SemaphoreType.DMA
    density_sums = (array(tiles + 1, 8, tile_size), vmem)
    force_sums = (array(tiles + 1, 16, tile_size), vmem)
    targets_out = (array(tiles + 1, 32, tile_size), vmem)
    lists = pltpu.SMEM((8, rows), jnp.int32)

    packed, codes = call(
        functools.partial(pack_kernel, tiles, tile_size, width_gy),
        "pack",
        [(array(tiles + 1, FIELDS, tile_size), vmem), (array(8, rows, dtype=jnp.int32), vmem)],
        [smem] + [hbm] * 4,
        [
            pltpu.SMEM((tiles,), jnp.int32),
            pltpu.VMEM((3 * tiles, tile_size), f32),
            pltpu.VMEM((tiles, tile_size), f32),
            pltpu.VMEM((2, rows), jnp.int32),
            dma((4,)),
        ],
    )(
        pair_count,
        *[
            pltpu.with_memory_space_constraint(operand, pltpu.HBM)
            for operand in (counts, points, mass.reshape(tiles, tile_size), pairs.T)
        ],
    )

    along_gx = swapped(packed, "gx")
    sums, targets = call(
        functools.partial(density_self_kernel, tiles), "density_self", [density_sums, targets_out], [vmem], [], tiles
    )(packed)
    sums, *along_gx = lax.optimization_barrier((sums, *along_gx))
    near = jnp.concatenate([packed] + along_gx, axis=0)
    even, odd = swapped(near, "gy")
    (sums,) = call(
        functools.partial(density_near_kernel, tiles), "density_near", [density_sums], [vmem] * 4, [lists, dma], tiles
    )(codes, sums, targets, near)
    density, extra, merged = call(
        functools.partial(density_kernel, tiles, tile_size),
        "density",
        [
            (array(tiles, tile_size), vmem),
            (array(tiles + tiles // 4, FIELDS, tile_size), vmem),
            (array(8 * rows, dtype=jnp.int32), smem),
        ],
        [hbm] + [vmem] * 8,
        [
            pltpu.VMEM((tiles + 1, 8, tile_size), f32),
            pltpu.VMEM((8, rows), jnp.int32),
            lists,
            pltpu.SMEM((tiles,), jnp.int32),
            dma((2,)),
        ],
        4 * tiles,
    )(counts, sums, targets, stiffness.reshape(tiles, tile_size), speeds, codes, near, even, odd)

    extra_gx = swapped(extra, "gx")
    (sums,) = call(
        functools.partial(force_self_kernel, tiles), "force_self", [force_sums], [vmem] * 3, [], tiles
    )(packed, targets, extra)
    sums, *extra_gx = lax.optimization_barrier((sums, *extra_gx))
    near_extra = jnp.concatenate([extra] + extra_gx, axis=0)
    even_extra, odd_extra = swapped(near_extra, "gy")
    (sums,) = call(
        functools.partial(force_near_kernel, tiles), "force_near", [force_sums], [vmem] * 5, [lists, dma], tiles
    )(codes, sums, targets, near, near_extra)
    new_points, new_speeds = call(
        functools.partial(force_kernel, tiles, tile_size),
        "force",
        [(array(3 * tiles, tile_size), vmem)] * 2,
        [hbm, smem] + [vmem] * 10,
        [pltpu.VMEM((tiles + 1, 16, tile_size), f32), pltpu.SMEM((tiles,), jnp.int32), dma],
        4 * tiles,
    )(counts, merged, sums, targets, points, speeds, near, even, odd, near_extra, even_extra, odd_extra)
    return (
        new_points.reshape(positions.shape),
        new_speeds.reshape(velocities.shape),
        density.reshape(mass.shape),
    )


def solution(mesh):
    placed = (
        P(None, "gx", "gy", None),
        P(None, "gx", "gy", None),
        P("gx", "gy", None),
        P("gx", "gy", None),
        P("gx", "gy", None),
        P(("gx", "gy"), None),
        P(("gx", "gy")),
    )
    return jax.shard_map(
        body,
        mesh=mesh,
        in_specs=placed,
        out_specs=(P(None, "gx", "gy", None), P(None, "gx", "gy", None), P("gx", "gy", None)),
        check_vma=False,
    )
```

```python
import functools
import math

import jax
import jax.numpy as jnp
from jax import lax
from jax.experimental import pallas as pl
from jax.experimental.pallas import tpu as pltpu
from jax.sharding import PartitionSpec as P


kernel_norm = 21.0 / (16.0 * math.pi)
viscosity = 0.1
time_step = 0.02
rest_density = 1.0
FIELDS = 4
UNROLL = 16
SENT = (1, 2, 4, 5)


def code_shift(tiles):
    return 1 << tiles.bit_length()


def swap_routes(axis):
    count = lax.axis_size(axis)
    routes = []
    for parity in (0, 1):
        route = []
        for i in range(parity, count - 1, 2):
            route += [(i, i + 1), (i + 1, i)]
        routes.append(route)
    return routes


def swapped(block, axis):
    return [lax.ppermute(block, axis, route) for route in swap_routes(axis)]


def split_int(value, size):
    if size & (size - 1) == 0:
        return value >> (size.bit_length() - 1), value & (size - 1)
    return lax.div(value, jnp.int32(size)), lax.rem(value, jnp.int32(size))


def partner_slot(step, here):
    even = lax.rem(here, 2) == 0
    up = jnp.where(even, 1, 2)
    return jnp.where(step == 0, 0, jnp.where(step > 0, up, 3 - up))


def fetch(sources, targets, sems):
    copies = [pltpu.make_async_copy(a, b, sems.at[i]) for i, (a, b) in enumerate(zip(sources, targets))]
    for copy in copies:
        copy.start()
    for copy in copies:
        copy.wait()


def pack_kernel(tiles, tile_size, width_gy, live_ref, counts_hbm, points_hbm, mass_hbm, pairs_hbm,
                packed_ref, codes_ref, valid_ref, counts_ref, points_ref, mass_ref, pairs_ref, sems):
    fetch(
        (counts_hbm, points_hbm, mass_hbm, pairs_hbm), (counts_ref, points_ref, mass_ref, pairs_ref), sems
    )
    rows = pairs_ref.shape[1]
    shift = code_shift(tiles)
    row_here, column_here = lax.axis_index("gx"), lax.axis_index("gy")
    lane = lax.broadcasted_iota(jnp.int32, (1, tile_size), 1)
    for t in range(tiles):
        for c in range(3):
            packed_ref[t, c : c + 1, :] = 0.5 * points_ref[c * tiles + t : c * tiles + t + 1, :] - 0.5
        valid = jnp.where(lane < counts_ref[t], 1.0, 0.0)
        valid_ref[t : t + 1, :] = valid
        packed_ref[t, 3:4, :] = mass_ref[t : t + 1, :] * valid
    box, slot = split_int(pairs_ref[...], tiles)
    box_gx, box_gy = split_int(box, width_gy)
    side_a = partner_slot(box_gx[0:1] - row_here, row_here)
    side_b = partner_slot(box_gy[1:2] - column_here, column_here)
    slot_a, slot_b = slot[0:1], slot[1:2]
    row_index = lax.broadcasted_iota(jnp.int32, (1, rows), 1)
    live = (row_index >= tiles) & (row_index < live_ref[0])
    cross = live & (pairs_ref[0:1] != pairs_ref[1:2])
    group_a = jnp.where(live, side_a, 7)
    group_b = jnp.where(cross, side_b + 3, 7)
    source_box = (side_b * 4 + side_a) * tiles
    code_a = (slot_a + shift * (source_box + slot_b)).astype(jnp.float32)
    code_b = (slot_b + shift * (source_box + slot_a)).astype(jnp.float32)
    sub = lax.broadcasted_iota(jnp.int32, (8, rows), 0)
    listed = ((sub == group_a) | (sub == group_b)) & (sub < 6)
    late = jnp.where(listed & (side_b == 2), 1.0, 0.0)
    early = jnp.where(listed & (side_b != 2), 1.0, 0.0)
    flags = jnp.concatenate([early, late], axis=0)
    lanes = lax.broadcasted_iota(jnp.int32, (rows, rows), 1)
    subs = lax.broadcasted_iota(jnp.int32, (rows, rows), 0)
    above = jnp.where(subs < lanes, 1.0, 0.0).astype(jnp.bfloat16)
    places = jnp.dot(flags.astype(jnp.bfloat16), above, preferred_element_type=jnp.float32)
    early_totals = jnp.sum(early, axis=1, keepdims=True)
    totals = early_totals + jnp.sum(late, axis=1, keepdims=True)
    places = jnp.where(early > 0.0, places[0:8], early_totals + places[8:16])
    columns = jnp.where(listed, places, -1.0).T
    codes = jnp.concatenate(split_terms(jnp.where(sub < 3, code_a, code_b), 2), axis=0)
    picked = lax.broadcasted_iota(jnp.int32, (8, 8 * rows), 0)
    picks = jnp.where(picked == lax.broadcasted_iota(jnp.int32, (8, 8 * rows), 1) // rows, 1.0, 0.0)
    spread = jnp.dot(columns, picks[:, : 6 * rows], preferred_element_type=jnp.float32)
    lanes = lanes.astype(jnp.float32)
    hits = jnp.concatenate(
        [
            jnp.where(spread[:, q * rows : (q + 1) * rows] == lanes, 1.0, 0.0).astype(jnp.bfloat16)
            for q in range(6)
        ],
        axis=1,
    )
    found = jnp.dot(codes, hits, preferred_element_type=jnp.float32)
    row_lane = lanes[0:1, :]
    codes_ref[...] = jnp.zeros(codes_ref.shape, jnp.int32)
    for q in range(6):
        here = slice(q * rows, (q + 1) * rows)
        code = found[q : q + 1, here] + found[8 + q : 9 + q, here]
        total = totals[q : q + 1, :]
        code = jnp.where(row_lane < total, code, float(tiles))
        code = jnp.where(row_lane == rows - 1, total, code)
        code = jnp.where(row_lane == rows - 2, early_totals[q : q + 1, :], code)
        codes_ref[q : q + 1, :] = code.astype(jnp.int32)
        if q in SENT:
            place = SENT.index(q)
            packed_ref[tiles, place : place + 1, :] = code


def split_terms(values, terms):
    parts = []
    rest = values
    for i in range(terms):
        part = rest.astype(jnp.bfloat16)
        parts.append(part)
        if i + 1 < terms:
            rest = rest - part.astype(jnp.float32)
    return parts


def point_terms(block):
    block = jnp.concatenate([block, block], axis=0)
    sub = lax.broadcasted_iota(jnp.int32, block.shape, 0)
    points = jnp.where(sub < 3, block, 0.0)
    first, second = [part.astype(jnp.float32) for part in split_terms(points, 2)]
    kept = first + second
    length = jnp.sum(kept * kept, axis=0, keepdims=True)
    rest = jnp.where(sub < 6, length, block[3:4, :])
    q1, q2, q3 = [part.astype(jnp.float32) for part in split_terms(rest, 3)]
    return sub, first, second, q1, q2, q3


def source_terms(block):
    sub, first, second, q1, q2, q3 = point_terms(block)
    top = jnp.where((sub == 3) | (sub == 6), q1, jnp.where(sub == 5, q3, q2))
    top = jnp.where(sub < 3, first, top)
    ones = jnp.where(sub < 3, first, jnp.where(sub == 6, q3, jnp.where(sub < 6, 1.0, 0.0)))
    return jnp.concatenate([top, ones, second, second], axis=0).T


def target_terms(block):
    sub, first, second, q1, q2, q3 = point_terms(block)
    first, second = -2.0 * first, -2.0 * second
    top = jnp.where(sub < 3, first, jnp.where(sub < 6, 1.0, 0.0))
    lengths = jnp.where(sub == 3, q1, jnp.where(sub == 4, q2, jnp.where(sub == 5, q3, second)))
    return jnp.concatenate([top, lengths, first, second], axis=0)


def mass_picks(tile_size):
    row = lax.broadcasted_iota(jnp.int32, (32, tile_size), 0)
    return jnp.where((row == 6) | (row == 7) | (row == 14), 1.0, 0.0)


def falloff_of(square):
    square = jnp.maximum(square, 1e-24)
    return jnp.maximum(1.0 - square * lax.rsqrt(square), 0.0)


def density_side(source_block, targets, picks):
    size = source_block.shape[1]
    both = jnp.dot(
        source_terms(source_block),
        jnp.concatenate([targets, picks], axis=1),
        preferred_element_type=jnp.float32,
    )
    total = None
    for j in range(0, size, 8):
        falloff = falloff_of(both[j : j + 8, 0:size])
        f2 = falloff * falloff
        term = f2 * f2 * ((1.25 - falloff) * both[j : j + 8, size:])
        total = term if total is None else total + term
    return total


def force_side(source_block, extra_block, last_speed, targets):
    size = source_block.shape[1]
    squares = jnp.dot(source_terms(source_block), targets, preferred_element_type=jnp.float32)
    high, low = [], []
    for j in range(0, size, 16):
        falloff = falloff_of(squares[j : j + 16])
        top, rest = split_terms(falloff * falloff * falloff, 2)
        high.append(top)
        low.append(rest)
    slope = jnp.concatenate(high + low, axis=0)
    base = jnp.concatenate([source_block, extra_block], axis=0)
    sub = lax.broadcasted_iota(jnp.int32, base.shape, 0)
    base = jnp.where((sub == 3) | (sub == 7), 1.0, jnp.where(sub == 6, last_speed, base))
    mass = source_block[3:4, :]
    mass_press = mass * extra_block[2:3, :]
    mass_inverse = mass * extra_block[3:4, :]
    columns = jnp.concatenate(
        [base * jnp.where(sub < 4, mass, mass_inverse), base * mass_press], axis=0
    )
    columns = jnp.concatenate(split_terms(columns, 3), axis=0)
    columns = jnp.concatenate([columns, columns], axis=1)
    sums = jnp.dot(columns, slope, preferred_element_type=jnp.float32)
    return sums[0:16] + sums[16:32] + sums[32:48]


def merge_lists(lists_ref, merged_ref, parts, dummy):
    last = lists_ref.shape[1] - 1
    start = jnp.int32(0)
    for row, early in parts:
        first = 0 if early else lists_ref[row, last - 1]
        count = lists_ref[row, last - 1] if early else lists_ref[row, last] - first

        def chunk(i, carry, row=row, first=first, start=start):
            for k in range(4):
                merged_ref[start + 4 * i + k] = lists_ref[row, first + 4 * i + k]
            return carry

        lax.fori_loop(0, (count + 3) // 4, chunk, 0)
        start = start + count
    for k in range(UNROLL):
        merged_ref[start + k] = dummy
    merged_ref[merged_ref.shape[0] - 1] = start


def each_side(count, code_at, tiles, one_side):
    shift = code_shift(tiles)

    def trip(i, carry):
        for u in range(UNROLL):
            code = code_at(i * UNROLL + u)
            one_side(code & (shift - 1), code >> (shift.bit_length() - 1))
        return carry

    lax.fori_loop(0, (count + UNROLL - 1) // UNROLL, trip, 0)


def merged_sides(merged_ref, tiles, one_side):
    count = merged_ref[merged_ref.shape[0] - 1]
    each_side(count, lambda k: merged_ref[k], tiles, one_side)


def each_tile(tiles, one_tile):
    def trip(i, carry):
        for u in range(UNROLL):
            one_tile(i * UNROLL + u)
        return carry

    lax.fori_loop(0, tiles // UNROLL, trip, 0)


def density_self_kernel(tiles, packed_ref, speeds_ref, sums_ref, targets_ref, extra_ref):
    picks = mass_picks(packed_ref.shape[2])

    def one_tile(t):
        block = packed_ref[t]
        targets = target_terms(block)
        targets_ref[t] = targets
        sums_ref[t] = density_side(block, targets, picks)

    each_tile(tiles, one_tile)
    sums_ref[tiles] = jnp.zeros(sums_ref.shape[1:], jnp.float32)
    targets_ref[tiles] = jnp.zeros(targets_ref.shape[1:], jnp.float32)
    for t in range(tiles):
        for c in range(2):
            extra_ref[t, c : c + 1, :] = speeds_ref[c * tiles + t : c * tiles + t + 1, :]
        extra_ref[tiles + t // 4, t % 4 : t % 4 + 1, :] = speeds_ref[2 * tiles + t : 2 * tiles + t + 1, :]


def place_of(source, tiles, extra_rows):
    box, slot = split_int(source, tiles)
    return box >= 4, (box & 3) * (tiles + extra_rows), slot


def take(refs, source, tiles, extra_rows):
    beyond, start, slot = place_of(source, tiles, extra_rows)
    blocks = [ref[start + slot] for ref in refs]
    return blocks[0] if len(refs) == 1 else jnp.where(beyond, blocks[1], blocks[0])


def take_speed(refs, source, tiles, extra_rows):
    beyond, start, slot = place_of(source, tiles, extra_rows)
    rows = [ref[start + tiles + (slot >> 2), pl.ds(slot & 3, 1), :] for ref in refs]
    return rows[0] if len(refs) == 1 else jnp.where(beyond, rows[1], rows[0])


def stage_lists(rows, lists_ref, codes_ref, sem):
    for q, row in enumerate(rows):
        lists_ref[q : q + 1, :] = row.astype(jnp.int32)
    lists_ref[len(rows) : 8, :] = jnp.zeros((8 - len(rows), lists_ref.shape[1]), jnp.int32)
    copy = pltpu.make_async_copy(lists_ref, codes_ref, sem)
    copy.start()
    return copy


def near_lists(codes_ref, near_ref, tiles):
    return [codes_ref[0:1, :]] + [near_ref[g * (tiles + 1) + tiles, g - 1 : g, :] for g in (1, 2)]


def density_early_kernel(tiles, codes_in_ref, sums_in_ref, targets_ref, near_ref, even_ref, sums_ref,
                         merged_ref, lists_ref, codes_ref, sem):
    rows = near_lists(codes_in_ref, near_ref, tiles) + [codes_in_ref[3:4, :], even_ref[tiles, 2:3, :]]
    copy = stage_lists(rows, lists_ref, codes_ref, sem)
    sums_ref[...] = sums_in_ref[...]
    copy.wait()
    merge_lists(codes_ref, merged_ref, [(q, True) for q in range(5)], tiles)
    picks = mass_picks(near_ref.shape[2])

    def one_side(target, source):
        block = take((near_ref, even_ref), source, tiles, 1)
        sums_ref[target] += density_side(block, targets_ref[target], picks)

    merged_sides(merged_ref, tiles, one_side)


def density_late_kernel(tiles, tile_size, sums_in_ref, targets_ref, stiff_ref, valid_ref, codes_in_ref,
                        near_ref, odd_ref, speeds_ref, density_ref, extra_ref, merged_ref, sums_ref,
                        lists_ref, codes_ref, sem):
    rows = near_lists(codes_in_ref, near_ref, tiles) + [odd_ref[tiles, 3:4, :]]
    copy = stage_lists(rows, lists_ref, codes_ref, sem)
    sums_ref[...] = sums_in_ref[...]
    extra_ref[...] = speeds_ref[...]
    copy.wait()
    merge_lists(codes_ref, merged_ref, [(q, False) for q in range(4)], tiles)
    picks = mass_picks(tile_size)

    def one_side(target, source):
        block = take((odd_ref,), source, tiles, 1)
        sums_ref[target] += density_side(block, targets_ref[target], picks)

    merged_sides(merged_ref, tiles, one_side)
    for t in range(tiles):
        density_ref[t : t + 1, :] = jnp.sum(sums_ref[t], axis=0, keepdims=True) * (4.0 * kernel_norm)
    total = density_ref[...]
    scale = total + 1.0 - valid_ref[...]
    press = stiff_ref[...] * (total - rest_density) / (scale * scale)
    inverse = 1.0 / scale
    for t in range(tiles):
        extra_ref[t, 2:3, :] = press[t : t + 1]
        extra_ref[t, 3:4, :] = inverse[t : t + 1]


def force_self_kernel(tiles, packed_ref, targets_ref, extra_ref, sums_ref):
    def one_tile(t):
        last_speed = take_speed((extra_ref,), t, tiles, tiles // 4)
        sums_ref[t] = force_side(packed_ref[t], extra_ref[t], last_speed, targets_ref[t])

    each_tile(tiles, one_tile)
    sums_ref[tiles] = jnp.zeros(sums_ref.shape[1:], jnp.float32)


def force_sides(merged_ref, tiles, blocks, extras, targets_ref, sums_ref):
    def one_side(target, source):
        block = take(blocks, source, tiles, 1)
        extra = take(extras, source, tiles, tiles // 4)
        last_speed = take_speed(extras, source, tiles, tiles // 4)
        sums_ref[target] += force_side(block, extra, last_speed, targets_ref[target])

    merged_sides(merged_ref, tiles, one_side)


def force_early_kernel(tiles, merged_ref, sums_in_ref, targets_ref, near_ref, even_ref, near_extra_ref,
                       even_extra_ref, sums_ref):
    sums_ref[...] = sums_in_ref[...]
    force_sides(
        merged_ref, tiles, (near_ref, even_ref), (near_extra_ref, even_extra_ref), targets_ref, sums_ref
    )


def force_late_kernel(tiles, merged_ref, sums_in_ref, targets_ref, points_ref, speeds_ref,
                      valid_ref, packed_ref, odd_ref, extra_ref, odd_extra_ref, points_out_ref,
                      speeds_out_ref, sums_ref):
    sums_ref[...] = sums_in_ref[...]
    force_sides(merged_ref, tiles, (odd_ref,), (odd_extra_ref,), targets_ref, sums_ref)
    push_here, drag_here = extra_ref[0:tiles, 2, :], extra_ref[0:tiles, 3, :]
    drag_here = (2.0 * viscosity) * drag_here
    step = (-5.0 * kernel_norm * time_step) * valid_ref[...]

    def column(c):
        return sums_ref[0:tiles, c, :]

    for c in range(3):
        rows = slice(c * tiles, (c + 1) * tiles)
        half_point = packed_ref[0:tiles, c, :]
        speed = speeds_ref[rows]
        push = push_here * (column(c) - half_point * column(3)) + (column(8 + c) - half_point * column(11))
        drag = drag_here * (speed * column(7) - column(4 + c))
        new_speed = speed + step * (2.0 * push + drag)
        speeds_out_ref[rows] = new_speed
        points_out_ref[rows] = points_ref[rows] + time_step * new_speed


def step_of(positions, velocities, mass, stiffness, counts, pairs, pair_count):
    tiles = counts.shape[2]
    slot_count = positions.shape[3]
    tile_size = slot_count // tiles
    rows = pairs.shape[0]
    width_gy = lax.axis_size("gy")
    points = positions.reshape(3 * tiles, tile_size)
    speeds = velocities.reshape(3 * tiles, tile_size)
    counts = counts.reshape(tiles)
    smem = pl.BlockSpec(memory_space=pltpu.SMEM)
    vmem = pl.BlockSpec(memory_space=pltpu.VMEM)
    hbm = pl.BlockSpec(memory_space=pltpu.HBM)
    f32 = jnp.float32

    def call(kernel, outs, ins, scratch, sides=0):
        params = dict(cost_estimate=pl.CostEstimate(
            flops=sides * 25 * tile_size * tile_size, transcendentals=0, bytes_accessed=1 << 20
        ))
        return pl.pallas_call(
            kernel,
            out_shape=tuple(out for out, _ in outs),
            in_specs=ins,
            out_specs=tuple(space for _, space in outs),
            scratch_shapes=scratch,
            compiler_params=pltpu.CompilerParams(vmem_limit_bytes=12 << 20),
            **params,
        )

    def array(*shape, dtype=f32):
        return jax.ShapeDtypeStruct(shape, dtype)

    dma = pltpu.SemaphoreType.DMA
    density_sums = (array(tiles + 1, 8, tile_size), vmem)
    force_sums = (array(tiles + 1, 16, tile_size), vmem)
    extra_out = (array(tiles + tiles // 4, FIELDS, tile_size), vmem)
    targets_out = (array(tiles + 1, 32, tile_size), vmem)

    packed, codes, valid = call(
        functools.partial(pack_kernel, tiles, tile_size, width_gy),
        [
            (array(tiles + 1, FIELDS, tile_size), vmem),
            (array(8, rows, dtype=jnp.int32), vmem),
            (array(tiles, tile_size), vmem),
        ],
        [smem] + [hbm] * 4,
        [
            pltpu.SMEM((tiles,), jnp.int32),
            pltpu.VMEM((3 * tiles, tile_size), f32),
            pltpu.VMEM((tiles, tile_size), f32),
            pltpu.VMEM((2, rows), jnp.int32),
            dma((4,)),
        ],
    )(
        pair_count,
        *[
            pltpu.with_memory_space_constraint(operand, pltpu.HBM)
            for operand in (counts, points, mass.reshape(tiles, tile_size), pairs.T)
        ],
    )

    along_gx = swapped(packed, "gx")
    sums, targets, speed_blocks = call(
        functools.partial(density_self_kernel, tiles), [density_sums, targets_out, extra_out], [vmem] * 2, [], tiles
    )(packed, speeds)
    sums, *along_gx = lax.optimization_barrier((sums, *along_gx))
    near = jnp.concatenate([packed] + along_gx, axis=0)
    even, odd = swapped(near, "gy")
    merged = (array(8 * rows, dtype=jnp.int32), smem)
    staged = [pltpu.VMEM((8, rows), jnp.int32), pltpu.SMEM((8, rows), jnp.int32)]
    sums, early = call(
        functools.partial(density_early_kernel, tiles), [density_sums, merged], [vmem] * 5, staged + [dma], 2 * tiles
    )(codes, sums, targets, near, even)
    density, extra, late = call(
        functools.partial(density_late_kernel, tiles, tile_size),
        [(array(tiles, tile_size), vmem), extra_out, merged],
        [vmem] * 8,
        [pltpu.VMEM((tiles + 1, 8, tile_size), f32)] + staged + [dma],
        2 * tiles,
    )(sums, targets, stiffness.reshape(tiles, tile_size), valid, codes, near, odd, speed_blocks)

    extra_gx = swapped(extra, "gx")
    (sums,) = call(
        functools.partial(force_self_kernel, tiles), [force_sums], [vmem] * 3, [], tiles
    )(packed, targets, extra)
    sums, *extra_gx = lax.optimization_barrier((sums, *extra_gx))
    near_extra = jnp.concatenate([extra] + extra_gx, axis=0)
    even_extra, odd_extra = swapped(near_extra, "gy")
    (sums,) = call(
        functools.partial(force_early_kernel, tiles), [force_sums], [smem] + [vmem] * 6, [], 2 * tiles
    )(early, sums, targets, near, even, near_extra, even_extra)
    new_points, new_speeds = call(
        functools.partial(force_late_kernel, tiles),
        [(array(3 * tiles, tile_size), vmem)] * 2,
        [smem] + [vmem] * 9,
        [pltpu.VMEM((tiles + 1, 16, tile_size), f32)],
        2 * tiles,
    )(late, sums, targets, points, speeds, valid, packed, odd, extra, odd_extra)
    return (
        new_points.reshape(positions.shape),
        new_speeds.reshape(velocities.shape),
        density.reshape(mass.shape),
    )


def solution(mesh):
    placed = (
        P(None, "gx", "gy", None),
        P(None, "gx", "gy", None),
        P("gx", "gy", None),
        P("gx", "gy", None),
        P("gx", "gy", None),
        P(("gx", "gy"), None),
        P(("gx", "gy")),
    )
    return jax.shard_map(
        step_of,
        mesh=mesh,
        in_specs=placed,
        out_specs=(P(None, "gx", "gy", None), P(None, "gx", "gy", None), P("gx", "gy", None)),
        check_vma=False,
    )
```
